32 devices in a mesh: grp: 4 (over y, core), dev: 8 (over z, x).
Axes of the slice: x: 2, y: 2, z: 4, core: 2. Of those that a mesh axis runs over, the one named last changes fastest.
Arguments:
- basis_values: bfloat16 [128, 256, 512], P(('grp', 'dev')), may hold values from -1 to 1
- stored_density_blocks: bfloat16 [64, 128, 128], P('dev'), may hold values from -0.5 to 0.5
- device_request: int32 [32, 8, 8], P(('grp', 'dev')), may hold values from -1 to 7, as said below
- batch_blocks: int32 [128, 16], P(('grp', 'dev')), may hold values from 0 to 63, as said below
- batch_atom: int32 [128], P(('grp', 'dev')), may hold values from 0 to 999
- point_offset: float32 [3, 128, 256], P(None, ('grp', 'dev')), may hold values from -8 to 8
- point_weight: float32 [128, 256], P(('grp', 'dev')), may hold values from 0.02 to 0.5
- exchange_kernel: float32 [128, 256], P(('grp', 'dev')), may hold values from -3 to -0.3
- atom_xyz: float32 [3, 1000], replicated, may hold values from -15 to 15
Outputs:
- response_hamiltonian: bfloat16 [64, 128, 128], P('dev')
- response_density: float32 [128, 256], P(('grp', 'dev'))
- multipoles: float32 [4, 1000], replicated
The draws below stay inside these ranges and needn't reach their ends.
Inputs may be any that keep to these rules, and one draw needn't show every extreme that they name: `device_request`: row d belongs to device d of grp+dev in grp-major order. Each row has exactly 32 entries other than -1, distinct for one owner; in every group one owner is asked for 8 blocks by every device of the group. `batch_blocks`: every entry points to an entry of its device's request row that is not -1.
All inputs are finite; a program needn't handle non-finite values.
Results may differ from the reference program's by a relative error of at most 0.004.
Values may be sent and summed in bfloat16 or wider, within the bound.
A program may use at most 64 MiB of HBM per device.

```python
import math
import jax
import jax.numpy as jnp
from jax import lax

TILE_FUNCTIONS = 128
REL = 4
PTS = 256
BATCH_DEV = 4
OWN_DEV = 8
NEED = 32
ATOMS = 1000
OWNERS = 8
CAP = 8
NBATCH = 128
STORED_BLOCKS = 64


def request_layout(key):
    device_list = NBATCH // BATCH_DEV
    positions = OWNERS * CAP
    hot = jax.random.randint(jax.random.fold_in(key, 11), (device_list // OWNERS,), 0, OWNERS)
    hot_device = jnp.repeat(hot, OWNERS)
    owner_of = jnp.arange(positions, dtype=jnp.int32) // CAP
    noise = jax.random.randint(jax.random.fold_in(key, 12), (device_list, positions), 1, 2 ** 20)
    index = jnp.arange(positions, dtype=jnp.int32)[None, :]
    score = jnp.where(owner_of[None, :] == hot_device[:, None], index, noise * positions + index)
    order = jnp.argsort(score, axis=1).astype(jnp.int32)
    rank = jnp.argsort(order, axis=1)
    live = rank < NEED
    shuffle = jax.random.randint(jax.random.fold_in(key, 13), (device_list, OWNERS, OWN_DEV), 0, 2 ** 20)
    rank_ordered = shuffle * OWN_DEV + jnp.arange(OWN_DEV, dtype=jnp.int32)
    picks = jnp.argsort(rank_ordered, axis=2)[:, :, :CAP].astype(jnp.int32)
    request = jnp.where(live.reshape(device_list, OWNERS, CAP), picks, -1).astype(jnp.int32)
    return (request, order[:, :NEED])


def draw_device_request(key, part):
    return request_layout(key)[0]


def draw_batch_blocks(key, part):
    request, live_positions = request_layout(key)
    device_list = NBATCH // BATCH_DEV
    chosen = jax.random.randint(jax.random.fold_in(key, 14), (device_list, BATCH_DEV * REL * REL), 0, NEED)
    picked = jnp.take_along_axis(live_positions, chosen, axis=1)
    return picked.reshape(NBATCH, REL * REL).astype(jnp.int32)


def with_ends(values, rng, smallest, high):
    index_at = [jax.random.randint(jax.random.fold_in(rng, axis), (), 0, length) for axis, length in enumerate(values.shape)]
    widest = values.shape.index(max(values.shape))
    next_to = index_at[:widest] + [(index_at[widest] + 1) % values.shape[widest]] + index_at[widest + 1:]
    return values.at[tuple(index_at)].set(smallest).at[tuple(next_to)].set(high)


def shard_levels(rng, extent, cuts, smallest, top_value):
    level, own = 1.0, jax.random.fold_in(rng, 6)
    for position, blocks in cuts:
        steps = jnp.exp(jax.random.uniform(jax.random.fold_in(own, position), (blocks,), jnp.float32, smallest / len(cuts), top_value / len(cuts)))
        level = level * jnp.repeat(steps, extent[position] // blocks).reshape([-1 if axis == position else 1 for axis in range(len(extent))])
    return level


def scatter_about(stream_key, dims, deviation, reach, pieces=(), kind=jnp.bfloat16):
    array = deviation * jax.random.normal(stream_key, dims, jnp.float32)
    if pieces:
        array = array * shard_levels(stream_key, dims, pieces, -0.22, 0.18)
    return jnp.clip(array, -reach, reach).astype(kind)


def setup_inputs(seed: int = 0) -> dict:
    keys = jax.random.split(jax.random.key(seed), 10)
    basis_values = scatter_about(keys[0], (NBATCH, PTS, REL * TILE_FUNCTIONS), 0.15, 1.0, ((0, 32),))
    stored_density_blocks = scatter_about(keys[1], (STORED_BLOCKS, TILE_FUNCTIONS, TILE_FUNCTIONS), TILE_FUNCTIONS ** -0.5, 0.5, ((0, 8),))
    device_request = draw_device_request(jax.random.fold_in(keys[9], 71), 0)
    batch_blocks = draw_batch_blocks(jax.random.fold_in(keys[9], 71), 0)
    batch_atom = with_ends(jax.random.randint(keys[4], (NBATCH,), 0, ATOMS), jax.random.fold_in(keys[4], 1), 0, ATOMS - 1).astype(jnp.int32)
    point_offset = scatter_about(keys[5], (3, NBATCH, PTS), 1.5, 8.0, ((1, 32),), jnp.float32)
    point_weight = jnp.clip(jnp.exp(math.log(0.5) - 3.218876 * jax.random.uniform(keys[6], (NBATCH, PTS), jnp.float32) ** shard_levels(keys[6], (NBATCH, PTS), ((0, 32),), -0.2, 0.2)), 0.02, 0.5)
    exchange_kernel = jnp.clip(-3.0 + 2.7 * jax.random.uniform(keys[7], (NBATCH, PTS), jnp.float32) ** shard_levels(keys[7], (NBATCH, PTS), ((0, 32),), -0.2, 0.2), -3.0, -0.3)
    atom_xyz = jnp.clip(jax.random.uniform(keys[8], (3, ATOMS), jnp.float32, -15.0, 15.0), -15.0, 15.0)
    return {"basis_values": basis_values, "stored_density_blocks": stored_density_blocks, "device_request": device_request, "batch_blocks": batch_blocks, "batch_atom": batch_atom, "point_offset": point_offset, "point_weight": point_weight, "exchange_kernel": exchange_kernel, "atom_xyz": atom_xyz}


HIGH = lax.Precision.HIGHEST

def far_field(multipoles, centre, offset, atom_xyz):
    gap = centre[:, None, None] + offset[:, :, None] - atom_xyz[:, None, :]
    inverse = lax.rsqrt(gap[0] * gap[0] + gap[1] * gap[1] + gap[2] * gap[2] + 1.0)
    cube = inverse * inverse * inverse
    dipole = multipoles[1] * gap[0] + multipoles[2] * gap[1] + multipoles[3] * gap[2]
    return lax.optimization_barrier(jnp.sum(multipoles[0] * inverse + dipole * cube, axis=1))

def reference(basis_values, stored_density_blocks, device_request, batch_blocks, batch_atom, point_offset, point_weight, exchange_kernel, atom_xyz):
    device_list, owners, capacity = device_request.shape
    own = stored_density_blocks.shape[0] // owners
    tile = stored_density_blocks.shape[1]
    batches, points, width = basis_values.shape
    rel = width // tile
    per_dev = batches // device_list
    atoms = atom_xyz.shape[1]
    owner_base = (jnp.arange(owners, dtype=jnp.int32) * own)[None, :, None]
    wanted = jnp.where(device_request >= 0, device_request + owner_base, -1).reshape(device_list, owners * capacity)
    batch_home = (jnp.arange(batches, dtype=jnp.int32) // per_dev).astype(jnp.int32)
    batch_slots = jnp.take_along_axis(wanted[batch_home], batch_blocks, axis=1)

    def density_one(args):
        values, slots = args
        blocks = stored_density_blocks[slots].astype(jnp.float32).reshape(rel, rel, tile, tile)
        split = values.astype(jnp.float32).reshape(points, rel, tile)
        left = jnp.einsum('rim,ijmn->rijn', split, blocks)
        return jnp.einsum('rijn,rjn->r', left, split)
    density_field = lax.map(density_one, (basis_values, batch_slots))
    weighted = density_field * point_weight
    parts = jnp.stack([lax.optimization_barrier(jnp.sum(weighted, 1)), lax.optimization_barrier(jnp.sum(weighted * point_offset[0], 1)), lax.optimization_barrier(jnp.sum(weighted * point_offset[1], 1)), lax.optimization_barrier(jnp.sum(weighted * point_offset[2], 1))])
    onehot = (batch_atom[:, None] == jnp.arange(atoms, dtype=jnp.int32)[None, :]).astype(jnp.float32)
    multipoles = jnp.dot(parts, onehot, precision=HIGH)
    centres = jnp.take(atom_xyz, batch_atom, axis=1)

    def potential_one(args):
        centre, offset = args
        return far_field(multipoles, centre, offset, atom_xyz)
    hartree = lax.map(potential_one, (centres.T, jnp.moveaxis(point_offset, 1, 0)))
    xc_part = point_weight * exchange_kernel * density_field
    hartree_part = point_weight * hartree

    def pair_terms(args):
        values, first, second = args
        wide = values.astype(jnp.float32)
        split = wide.reshape(points, rel, tile)
        one = (wide * first[:, None]).astype(jnp.bfloat16).astype(jnp.float32).reshape(points, rel, tile)
        two = (wide * second[:, None]).astype(jnp.bfloat16).astype(jnp.float32).reshape(points, rel, tile)
        return jnp.einsum('rim,rjn->ijmn', one, split) + jnp.einsum('rim,rjn->ijmn', two, split)

    def per_device(total, args):
        values, first, second, positions, requested_row = args
        terms = lax.map(pair_terms, (values, first, second))
        summed = jax.ops.segment_sum(terms.reshape(per_dev * rel * rel, tile * tile), positions.reshape(-1), num_segments=owners * capacity)
        rounded = lax.optimization_barrier(summed.astype(jnp.bfloat16)).astype(jnp.float32)
        target = jnp.where(requested_row >= 0, requested_row, total.shape[0]).astype(jnp.int32)
        return (total.at[target].add(rounded, mode='drop'), None)
    start_total = jnp.zeros((owners * own, tile * tile), jnp.float32)
    total, _ = lax.scan(per_device, start_total, (basis_values.reshape(device_list, per_dev, points, width), xc_part.reshape(device_list, per_dev, points), hartree_part.reshape(device_list, per_dev, points), batch_blocks.reshape(device_list, per_dev, rel * rel), wanted))
    hamiltonian = total.astype(jnp.bfloat16).reshape(owners * own, tile, tile)
    return (hamiltonian, density_field, multipoles)
```

```python
import functools

import jax
import jax.numpy as jnp
from jax import lax
from jax.experimental import pallas as pl
from jax.experimental.pallas import tpu as pltpu
from jax.sharding import PartitionSpec as P

MESH = pl.DeviceIdType.MESH
LANES = 128
VMEM = pl.BlockSpec(memory_space=pltpu.VMEM)
SMEM = pl.BlockSpec(memory_space=pltpu.SMEM)
ANY = pl.BlockSpec(memory_space=pl.ANY)
F32 = jnp.float32
BF16 = jnp.bfloat16


def remote(src, dst, send, recv, grp, dev):
    return pltpu.make_async_remote_copy(
        src_ref=src,
        dst_ref=dst,
        send_sem=send,
        recv_sem=recv,
        device_id=(grp, dev),
        device_id_type=MESH,
    )


def meet(peers):
    barrier = pltpu.get_barrier_semaphore()
    for grp, dev in peers:
        pl.semaphore_signal(barrier, inc=1, device_id=(grp, dev), device_id_type=MESH)
    pl.semaphore_wait(barrier, len(peers))


def slot_of(request, blocks, b, p, capacity, own):
    position = blocks[b, p]
    return (position // capacity) * own + request[position]


def density_kernel(
    groups,
    devs,
    capacity,
    stored,
    request,
    blocks,
    batch_atom,
    offset,
    weight,
    xyz,
    values_any,
    density,
    own_rows,
    table_out,
    values,
    gathered,
    table,
    local_sem,
    send_a,
    recv_a,
    send_b,
    recv_b,
    send_c,
    recv_c,
    send_d,
    recv_d,
):
    g, me = lax.axis_index("grp"), lax.axis_index("dev")
    own, tile = stored.shape[0], stored.shape[1]
    batches, points, width = values.shape
    rel = width // tile
    atoms = xyz.shape[1]
    half = own // 2
    core = lax.rem(g, 2)
    pair = g + 1 - 2 * core

    load = pltpu.make_async_copy(values_any, values, local_sem.at[0])
    load.start()
    mine = pltpu.make_async_copy(
        stored, gathered.at[pl.ds(me * own, own)], local_sem.at[1]
    )
    mine.start()
    peers = [(g, lax.rem(me + k, devs)) for k in range(1, devs)]
    peers += [(lax.rem(g + j, groups), me) for j in range(1, groups)]
    meet(peers)

    out = []
    for k in range(1, devs):
        copy = remote(
            stored.at[pl.ds(core * half, half)],
            gathered.at[pl.ds(me * own + core * half, half)],
            send_a.at[k],
            recv_a.at[k],
            g,
            lax.rem(me + k, devs),
        )
        copy.start()
        out.append(copy)

    centres = []
    spot = lax.broadcasted_iota(jnp.int32, (3, atoms), 1)
    for b in range(batches):
        centres.append(
            jnp.sum(jnp.where(spot == batch_atom[b], xyz[...], 0.0), axis=1, keepdims=True)
        )

    passed = []
    for k in range(1, devs):
        out[k - 1].wait_recv()
        rows = pl.ds(lax.rem(me + devs - k, devs) * own + core * half, half)
        copy = remote(
            gathered.at[rows], gathered.at[rows], send_b.at[k], recv_b.at[k], pair, me
        )
        copy.start()
        passed.append(copy)
    load.wait()
    mine.wait()
    for copy in passed:
        copy.wait_recv()

    lane = lax.broadcasted_iota(jnp.int32, (1, LANES), 1)
    for b in range(batches):
        matrix = jnp.concatenate(
            [
                jnp.concatenate(
                    [
                        gathered[slot_of(request, blocks, b, i * rel + j, capacity, own)]
                        for j in range(rel)
                    ],
                    axis=1,
                )
                for i in range(rel)
            ],
            axis=0,
        )
        left = jnp.dot(values[b], matrix, preferred_element_type=F32)
        product = left * values[b].astype(F32)
        folded = product[:, :tile]
        for i in range(1, rel):
            folded = folded + product[:, i * tile : (i + 1) * tile]
        row = jnp.sum(folded.T, axis=0, keepdims=True)
        density[pl.ds(b, 1), :] = row
        weighted = row * weight[pl.ds(b, 1), :]
        parts = [jnp.sum(weighted, axis=1, keepdims=True)]
        for k in range(3):
            parts.append(
                jnp.sum(weighted * offset[k, pl.ds(b, 1), :], axis=1, keepdims=True)
            )
        parts += [centres[b][k : k + 1] for k in range(3)]
        entry = jnp.zeros((1, LANES), F32) + batch_atom[b].astype(F32)
        for k, part in enumerate(parts):
            entry = jnp.where(lane == k, part, entry)
        own_rows[pl.ds(b, 1), :] = entry
        table[me, g, pl.ds(b, 1), :] = entry

    first = []
    for j in range(1, groups):
        copy = remote(
            table.at[me, g],
            table.at[me, g],
            send_c.at[j],
            recv_c.at[j],
            lax.rem(g + j, groups),
            me,
        )
        copy.start()
        first.append(copy)
    for copy in first:
        copy.wait_recv()
    second = []
    for k in range(1, devs):
        copy = remote(
            table.at[me], table.at[me], send_d.at[k], recv_d.at[k], g, lax.rem(me + k, devs)
        )
        copy.start()
        second.append(copy)
    for copy in out + passed + first:
        copy.wait_send()
    for copy in second:
        copy.wait_recv()
    for copy in second:
        copy.wait_send()
    for d in range(devs):
        table_out[d * groups : (d + 1) * groups] = table[d]


def term_kernel(
    capacity,
    own,
    request,
    blocks,
    values,
    table,
    own_rows,
    density,
    weight,
    exchange,
    offset,
    part,
    multipoles,
    total,
):
    batches, points, width = values.shape
    tile = part.shape[1]
    rel = width // tile
    devices = table.shape[0]
    atoms = multipoles.shape[1]
    chunk = min(devices, 32)
    total[...] = jnp.zeros_like(total)

    places = [
        [own_rows[pl.ds(b, 1), 4 + k : 5 + k] + offset[k, pl.ds(b, 1), :] for k in range(3)]
        for b in range(batches)
    ]
    spot = lax.broadcasted_iota(jnp.int32, (1, atoms), 1).astype(F32)

    def gather(step, carry):
        fields, moments = carry
        fields, moments = list(fields), list(moments)
        for source in range(batches):
            rows = table[pl.ds(step * chunk, chunk), source, :]
            column = [rows[:, k : k + 1] for k in range(8)]
            hit = column[7] == spot
            for k in range(4):
                moments[k] = moments[k] + jnp.sum(
                    jnp.where(hit, column[k], 0.0), axis=0, keepdims=True
                )
            for b in range(batches):
                gap = [places[b][k] - column[4 + k] for k in range(3)]
                inverse = lax.rsqrt(
                    gap[0] * gap[0] + gap[1] * gap[1] + gap[2] * gap[2] + 1.0
                )
                cube = inverse * inverse * inverse
                dipole = column[1] * gap[0] + column[2] * gap[1] + column[3] * gap[2]
                fields[b] = fields[b] + jnp.sum(
                    column[0] * inverse + dipole * cube, axis=0, keepdims=True
                )
        return tuple(fields), tuple(moments)

    carry = (
        tuple(jnp.zeros((1, points), F32) for _ in range(batches)),
        tuple(jnp.zeros((1, atoms), F32) for _ in range(4)),
    )
    if devices == chunk:
        fields, moments = gather(0, carry)
    else:
        fields, moments = lax.fori_loop(0, devices // chunk, gather, carry)
    for k in range(4):
        multipoles[pl.ds(k, 1), :] = moments[k]

    for b in range(batches):
        pick = pl.ds(b, 1)
        factors = (
            weight[pick, :] * exchange[pick, :] * density[pick, :],
            weight[pick, :] * fields[b],
        )
        wide = values[b].astype(F32)
        scaled = []
        for factor in factors:
            column = jnp.broadcast_to(factor, (tile, points)).T
            scaled.append(
                jnp.concatenate(
                    [
                        (wide[:, i * tile : (i + 1) * tile] * column).astype(BF16)
                        for i in range(rel)
                    ],
                    axis=1,
                )
            )
        stacked = jnp.concatenate(scaled, axis=0)
        doubled = jnp.concatenate([values[b], values[b]], axis=0)
        term = lax.dot_general(
            stacked, doubled, (((0,), (0,)), ((), ())), preferred_element_type=F32
        )
        for i in range(rel):
            for j in range(rel):
                slot = slot_of(request, blocks, b, i * rel + j, capacity, own)
                total[slot] += term[i * tile : (i + 1) * tile, j * tile : (j + 1) * tile]
    part[...] = total[...].astype(BF16)


def reduce_kernel(
    groups,
    devs,
    part,
    result,
    paired,
    outgoing,
    arrived,
    across,
    final,
    send_a,
    recv_a,
    send_b,
    recv_b,
    send_c,
    recv_c,
    send_d,
    recv_d,
):
    g, me = lax.axis_index("grp"), lax.axis_index("dev")
    own = result.shape[0]
    half = own // 2
    lines = groups // 2
    core = lax.rem(g, 2)
    line = g // 2
    pair = g + 1 - 2 * core

    peers = [(pair, me)]
    peers += [(g, lax.rem(me + k, devs)) for k in range(1, devs)]
    peers += [(lax.rem(line + j, lines) * 2 + core, me) for j in range(1, lines)]
    meet(peers)

    order = list(range(1, devs)) + [0]
    halves = {}
    for k in order:
        owner = lax.rem(me + k, devs)
        copy = remote(
            part.at[pl.ds(owner * own + (1 - core) * half, half)],
            paired.at[k],
            send_a.at[k],
            recv_a.at[k],
            pair,
            me,
        )
        copy.start()
        halves[k] = copy

    def sum_of_pair(k):
        owner = lax.rem(me + k, devs)
        here = part[pl.ds(owner * own + core * half, half)]
        return here.astype(F32) + paired[k].astype(F32)

    out = []
    for k in range(1, devs):
        halves[k].wait_recv()
        outgoing[k] = sum_of_pair(k).astype(BF16)
        copy = remote(
            outgoing.at[k],
            arrived.at[k],
            send_b.at[k],
            recv_b.at[k],
            g,
            lax.rem(me + k, devs),
        )
        copy.start()
        out.append(copy)
    halves[0].wait_recv()
    summed = sum_of_pair(0)
    for k in range(1, devs):
        out[k - 1].wait_recv()
        summed = summed + arrived[k].astype(F32)
    across[line] = summed.astype(BF16)
    rows = []
    for j in range(1, lines):
        copy = remote(
            across.at[line],
            across.at[line],
            send_c.at[j],
            recv_c.at[j],
            lax.rem(line + j, lines) * 2 + core,
            me,
        )
        copy.start()
        rows.append(copy)
    for copy in rows:
        copy.wait_recv()
    whole = across[0].astype(F32)
    for j in range(1, lines):
        whole = whole + across[j].astype(F32)
    final[pl.ds(core * half, half)] = whole.astype(BF16)
    last = remote(
        final.at[pl.ds(core * half, half)],
        final.at[pl.ds(core * half, half)],
        send_d,
        recv_d,
        pair,
        me,
    )
    last.start()
    for copy in list(halves.values()) + out + rows:
        copy.wait_send()
    last.wait_recv()
    last.wait_send()
    result[...] = final[...]


def on_device(
    groups,
    devs,
    basis_values,
    stored_density_blocks,
    device_request,
    batch_blocks,
    batch_atom,
    point_offset,
    point_weight,
    exchange_kernel,
    atom_xyz,
):
    batches, points, width = basis_values.shape
    own, tile = stored_density_blocks.shape[:2]
    owners, capacity = device_request.shape[1:]
    slots = devs * own
    atoms = atom_xyz.shape[1]
    half = own // 2
    request = device_request.reshape(owners * capacity)
    dma = pltpu.SemaphoreType.DMA

    density, own_rows, table = pl.pallas_call(
        functools.partial(density_kernel, groups, devs, capacity),
        out_shape=(
            jax.ShapeDtypeStruct((batches, points), F32),
            jax.ShapeDtypeStruct((batches, LANES), F32),
            jax.ShapeDtypeStruct((devs * groups, batches, LANES), F32),
        ),
        in_specs=[VMEM, SMEM, SMEM, SMEM, VMEM, VMEM, VMEM, ANY],
        out_specs=(VMEM, VMEM, VMEM),
        scratch_shapes=[
            pltpu.VMEM((batches, points, width), BF16),
            pltpu.VMEM((slots, tile, tile), BF16),
            pltpu.VMEM((devs, groups, batches, LANES), F32),
            dma((2,)),
            dma((devs,)),
            dma((devs,)),
            dma((devs,)),
            dma((devs,)),
            dma((groups,)),
            dma((groups,)),
            dma((devs,)),
            dma((devs,)),
        ],
        compiler_params=pltpu.CompilerParams(collective_id=0, has_side_effects=True),
    )(
        stored_density_blocks,
        request,
        batch_blocks,
        batch_atom,
        point_offset,
        point_weight,
        atom_xyz,
        basis_values,
    )

    part, multipoles = pl.pallas_call(
        functools.partial(term_kernel, capacity, own),
        out_shape=(
            jax.ShapeDtypeStruct((slots, tile, tile), BF16),
            jax.ShapeDtypeStruct((4, atoms), F32),
        ),
        in_specs=[SMEM, SMEM, VMEM, VMEM, VMEM, VMEM, VMEM, VMEM, VMEM],
        out_specs=(VMEM, VMEM),
        scratch_shapes=[pltpu.VMEM((slots, tile, tile), F32)],
    )(
        request,
        batch_blocks,
        basis_values,
        table,
        own_rows,
        density,
        point_weight,
        exchange_kernel,
        point_offset,
    )

    hamiltonian = pl.pallas_call(
        functools.partial(reduce_kernel, groups, devs),
        out_shape=jax.ShapeDtypeStruct((own, tile, tile), BF16),
        in_specs=[VMEM],
        out_specs=VMEM,
        scratch_shapes=[
            pltpu.VMEM((devs, half, tile, tile), BF16),
            pltpu.VMEM((devs, half, tile, tile), BF16),
            pltpu.VMEM((devs, half, tile, tile), BF16),
            pltpu.VMEM((groups // 2, half, tile, tile), BF16),
            pltpu.VMEM((own, tile, tile), BF16),
            dma((devs,)),
            dma((devs,)),
            dma((devs,)),
            dma((devs,)),
            dma((groups // 2,)),
            dma((groups // 2,)),
            dma,
            dma,
        ],
        compiler_params=pltpu.CompilerParams(collective_id=1, has_side_effects=True),
    )(part)
    return (hamiltonian, density, multipoles)


def solution(mesh):
    return jax.shard_map(
        functools.partial(on_device, mesh.shape["grp"], mesh.shape["dev"]),
        mesh=mesh,
        in_specs=(
            P(("grp", "dev"), None, None),
            P("dev", None, None),
            P(("grp", "dev"), None, None),
            P(("grp", "dev"), None),
            P(("grp", "dev")),
            P(None, ("grp", "dev"), None),
            P(("grp", "dev"), None),
            P(("grp", "dev"), None),
            P(),
        ),
        out_specs=(P("dev", None, None), P(("grp", "dev"), None), P()),
        check_vma=False,
    )
```

```python
import functools

import jax
import jax.numpy as jnp
from jax import lax
from jax.experimental import pallas as pl
from jax.experimental.pallas import tpu as pltpu
from jax.sharding import PartitionSpec as P

MESH = pl.DeviceIdType.MESH
LANES = 128
VMEM = pl.BlockSpec(memory_space=pltpu.VMEM)
SMEM = pl.BlockSpec(memory_space=pltpu.SMEM)
ANY = pl.BlockSpec(memory_space=pl.ANY)
F32 = jnp.float32
BF16 = jnp.bfloat16


def remote(src, dst, send, recv, grp, dev):
    return pltpu.make_async_remote_copy(
        src_ref=src,
        dst_ref=dst,
        send_sem=send,
        recv_sem=recv,
        device_id=(grp, dev),
        device_id_type=MESH,
    )


def meet(peers):
    barrier = pltpu.get_barrier_semaphore()
    for grp, dev in peers:
        pl.semaphore_signal(barrier, inc=1, device_id=(grp, dev), device_id_type=MESH)
    pl.semaphore_wait(barrier, len(peers))


def slot_of(request, blocks, b, p, capacity, own):
    position = blocks[b, p]
    owner = position // capacity
    return owner * own + request[0, owner, position - owner * capacity]


def flip(index, mask):
    out = index
    bit = 1
    while bit <= mask:
        if mask & bit:
            out = out + bit - 2 * bit * lax.rem(index // bit, 2)
        bit *= 2
    return out


def density_kernel(
    groups,
    devs,
    capacity,
    stored,
    request,
    blocks,
    batch_atom,
    offset,
    weight,
    xyz,
    values_any,
    density,
    own_rows,
    table_out,
    values,
    gathered,
    table,
    local_sem,
    send_a,
    recv_a,
    send_y,
    recv_y,
    send_b,
    recv_b,
    send_c,
    recv_c,
    send_d,
    recv_d,
):
    g, me = lax.axis_index("grp"), lax.axis_index("dev")
    own, tile = stored.shape[0], stored.shape[1]
    batches, points, width = values.shape
    rel = width // tile
    atoms = xyz.shape[1]
    half, quarter = own // 2, own // 4
    first_row = lax.rem(g, 2) * half
    lane_row = first_row + lax.rem(g // 2, 2) * quarter

    load = pltpu.make_async_copy(values_any, values, local_sem.at[0])
    load.start()
    mine = pltpu.make_async_copy(
        stored, gathered.at[pl.ds(me * own, own)], local_sem.at[1]
    )
    mine.start()
    peers = [(g, lax.rem(me + k, devs)) for k in range(1, devs)]
    peers += [(lax.rem(g + j, groups), me) for j in range(1, groups)]
    meet(peers)

    def piece(k):
        return pl.ds(flip(me, k) * own + lane_row, quarter)

    def source(k):
        return stored.at[pl.ds(lane_row, quarter)] if k == 0 else gathered.at[piece(k)]

    came = {}

    def onward(k):
        came[k + 1] = remote(
            source(k),
            gathered.at[piece(k)],
            send_a.at[k + 1],
            recv_a.at[k + 1],
            g,
            flip(me, 1),
        )
        came[k + 1].start()

    onward(0)
    for k in range(2, devs, 2):
        came[k] = remote(
            source(0), gathered.at[piece(0)], send_a.at[k], recv_a.at[k], g, flip(me, k)
        )
        came[k].start()

    centres = []
    spot = lax.broadcasted_iota(jnp.int32, (3, atoms), 1)
    for b in range(batches):
        centres.append(
            jnp.sum(jnp.where(spot == batch_atom[b], xyz[...], 0.0), axis=1, keepdims=True)
        )

    order = []
    for k in range(2, devs, 2):
        order += [k, k - 1]
    order.append(devs - 1)
    sideways, passed = {}, []

    def hand_over(k):
        sideways[k].wait_recv()
        rows = pl.ds(flip(me, k) * own + first_row, half)
        copy = remote(
            gathered.at[rows], gathered.at[rows], send_b.at[k], recv_b.at[k], flip(g, 1), me
        )
        copy.start()
        passed.append(copy)

    for step, k in enumerate(order):
        came[k].wait_recv()
        sideways[k] = remote(
            gathered.at[piece(k)],
            gathered.at[piece(k)],
            send_y.at[k],
            recv_y.at[k],
            flip(g, 2),
            me,
        )
        sideways[k].start()
        if k % 2 == 0:
            onward(k)
        if step >= 2:
            hand_over(order[step - 2])
    for k in order[-2:]:
        hand_over(k)
    out = list(came.values()) + list(sideways.values())
    load.wait()
    mine.wait()
    for copy in passed:
        copy.wait_recv()

    lane = lax.broadcasted_iota(jnp.int32, (1, LANES), 1)
    for b in range(batches):
        matrix = jnp.concatenate(
            [
                jnp.concatenate(
                    [
                        gathered[slot_of(request, blocks, b, i * rel + j, capacity, own)]
                        for j in range(rel)
                    ],
                    axis=1,
                )
                for i in range(rel)
            ],
            axis=0,
        )
        left = jnp.dot(values[b], matrix, preferred_element_type=F32)
        product = left * values[b].astype(F32)
        folded = product[:, :tile]
        for i in range(1, rel):
            folded = folded + product[:, i * tile : (i + 1) * tile]
        row = jnp.sum(folded.T, axis=0, keepdims=True)
        density[pl.ds(b, 1), :] = row
        weighted = row * weight[pl.ds(b, 1), :]
        parts = [jnp.sum(weighted, axis=1, keepdims=True)]
        for k in range(3):
            parts.append(
                jnp.sum(weighted * offset[k, pl.ds(b, 1), :], axis=1, keepdims=True)
            )
        parts += [centres[b][k : k + 1] for k in range(3)]
        entry = jnp.zeros((1, LANES), F32) + batch_atom[b].astype(F32)
        for k, part in enumerate(parts):
            entry = jnp.where(lane == k, part, entry)
        own_rows[pl.ds(b, 1), :] = entry
        table[me, g, pl.ds(b, 1), :] = entry

    first = []
    for j in range(1, groups):
        copy = remote(
            table.at[me, g],
            table.at[me, g],
            send_c.at[j],
            recv_c.at[j],
            lax.rem(g + j, groups),
            me,
        )
        copy.start()
        first.append(copy)
    for copy in first:
        copy.wait_recv()
    second = []
    for k in range(1, devs):
        copy = remote(
            table.at[me], table.at[me], send_d.at[k], recv_d.at[k], g, lax.rem(me + k, devs)
        )
        copy.start()
        second.append(copy)
    for copy in out + passed + first:
        copy.wait_send()
    for copy in second:
        copy.wait_recv()
    for copy in second:
        copy.wait_send()
    for d in range(devs):
        table_out[d * groups : (d + 1) * groups] = table[d]


def term_kernel(
    capacity,
    own,
    request,
    blocks,
    values,
    table,
    own_rows,
    density,
    weight,
    exchange,
    offset,
    part,
    multipoles,
    density_out,
    total,
):
    batches, points, width = values.shape
    tile = part.shape[1]
    rel = width // tile
    devices = table.shape[0]
    atoms = multipoles.shape[1]
    chunk = min(devices, 32)
    total[...] = jnp.zeros_like(total)
    density_out[...] = density[...]

    places = [
        [own_rows[pl.ds(b, 1), 4 + k : 5 + k] + offset[k, pl.ds(b, 1), :] for k in range(3)]
        for b in range(batches)
    ]
    spot = lax.broadcasted_iota(jnp.int32, (1, atoms), 1).astype(F32)

    def gather(step, carry):
        fields, moments = carry
        fields, moments = list(fields), list(moments)
        for source in range(batches):
            rows = table[pl.ds(step * chunk, chunk), source, :]
            column = [rows[:, k : k + 1] for k in range(8)]
            hit = column[7] == spot
            for k in range(4):
                moments[k] = moments[k] + jnp.sum(
                    jnp.where(hit, column[k], 0.0), axis=0, keepdims=True
                )
            for b in range(batches):
                gap = [places[b][k] - column[4 + k] for k in range(3)]
                inverse = lax.rsqrt(
                    gap[0] * gap[0] + gap[1] * gap[1] + gap[2] * gap[2] + 1.0
                )
                cube = inverse * inverse * inverse
                dipole = column[1] * gap[0] + column[2] * gap[1] + column[3] * gap[2]
                fields[b] = fields[b] + jnp.sum(
                    column[0] * inverse + dipole * cube, axis=0, keepdims=True
                )
        return tuple(fields), tuple(moments)

    carry = (
        tuple(jnp.zeros((1, points), F32) for _ in range(batches)),
        tuple(jnp.zeros((1, atoms), F32) for _ in range(4)),
    )
    if devices == chunk:
        fields, moments = gather(0, carry)
    else:
        fields, moments = lax.fori_loop(0, devices // chunk, gather, carry)
    for k in range(4):
        multipoles[pl.ds(k, 1), :] = moments[k]

    for b in range(batches):
        pick = pl.ds(b, 1)
        factors = (
            weight[pick, :] * exchange[pick, :] * density[pick, :],
            weight[pick, :] * fields[b],
        )
        wide = values[b].astype(F32)
        scaled = []
        for factor in factors:
            column = jnp.broadcast_to(factor, (tile, points)).T
            scaled.append(
                jnp.concatenate(
                    [
                        (wide[:, i * tile : (i + 1) * tile] * column).astype(BF16)
                        for i in range(rel)
                    ],
                    axis=1,
                )
            )
        stacked = jnp.concatenate(scaled, axis=0)
        doubled = jnp.concatenate([values[b], values[b]], axis=0)
        term = lax.dot_general(
            stacked, doubled, (((0,), (0,)), ((), ())), preferred_element_type=F32
        )
        for i in range(rel):
            for j in range(rel):
                slot = slot_of(request, blocks, b, i * rel + j, capacity, own)
                total[slot] += term[i * tile : (i + 1) * tile, j * tile : (j + 1) * tile]
    part[...] = total[...].astype(BF16)


def reduce_kernel(
    groups,
    devs,
    part,
    result,
    paired,
    sent_y,
    came_y,
    outgoing,
    arrived,
    across,
    final,
    send_a,
    recv_a,
    send_y,
    recv_y,
    send_b,
    recv_b,
    send_c,
    recv_c,
    send_d,
    recv_d,
):
    g, me = lax.axis_index("grp"), lax.axis_index("dev")
    own = result.shape[0]
    half, quarter = own // 2, own // 4
    quads = groups // 4
    quad, lane = g // 4, lax.rem(g, 4)
    core, side = lax.rem(g, 2), lax.rem(g // 2, 2)
    pair, beside = flip(g, 1), flip(g, 2)

    peers = [(pair, me), (beside, me)]
    peers += [(g, flip(me, k)) for k in range(1, devs)]
    peers += [(lax.rem(quad + j, quads) * 4 + lane, me) for j in range(1, quads)]
    meet(peers)

    order = list(range(devs - 1, -1, -1))
    halves, rows, out = {}, {}, {}
    for k in order:
        halves[k] = remote(
            part.at[pl.ds(flip(me, k) * own + (1 - core) * half, half)],
            paired.at[k],
            send_a.at[k],
            recv_a.at[k],
            pair,
            me,
        )
        halves[k].start()

    def sum_of_pair(k, which):
        here = part[pl.ds(flip(me, k) * own + core * half + which * quarter, quarter)]
        there = paired[k, pl.ds(which * quarter, quarter)]
        return here.astype(F32) + there.astype(F32)

    def sum_of_four(k):
        rows[k].wait_recv()
        return sum_of_pair(k, side) + came_y[k].astype(F32)

    def to_owner(k):
        outgoing[k] = sum_of_four(k).astype(BF16)
        out[k] = remote(
            outgoing.at[k], arrived.at[k], send_b.at[k], recv_b.at[k], g, flip(me, k)
        )
        out[k].start()

    for step, k in enumerate(order):
        halves[k].wait_recv()
        sent_y[k] = sum_of_pair(k, 1 - side).astype(BF16)
        rows[k] = remote(
            sent_y.at[k], came_y.at[k], send_y.at[k], recv_y.at[k], beside, me
        )
        rows[k].start()
        if step >= 2:
            to_owner(order[step - 2])
    to_owner(1)
    whole = sum_of_four(0)
    for k in order[:-1]:
        out[k].wait_recv()
        whole = whole + arrived[k].astype(F32)
    others = []
    if quads > 1:
        across[quad] = whole.astype(BF16)
        for j in range(1, quads):
            copy = remote(
                across.at[quad],
                across.at[quad],
                send_c.at[j],
                recv_c.at[j],
                lax.rem(quad + j, quads) * 4 + lane,
                me,
            )
            copy.start()
            others.append(copy)
        for copy in others:
            copy.wait_recv()
        whole = across[0].astype(F32)
        for j in range(1, quads):
            whole = whole + across[j].astype(F32)
    part_rows = pl.ds(core * half + side * quarter, quarter)
    half_rows = pl.ds(core * half, half)
    final[part_rows] = whole.astype(BF16)
    for step, (where, to) in enumerate(((part_rows, beside), (half_rows, pair))):
        copy = remote(
            final.at[where], final.at[where], send_d.at[step], recv_d.at[step], to, me
        )
        copy.start()
        copy.wait_recv()
        others.append(copy)
    for copy in [*halves.values(), *rows.values(), *out.values(), *others]:
        copy.wait_send()
    result[...] = final[...]


def on_device(
    groups,
    devs,
    basis_values,
    stored_density_blocks,
    device_request,
    batch_blocks,
    batch_atom,
    point_offset,
    point_weight,
    exchange_kernel,
    atom_xyz,
):
    batches, points, width = basis_values.shape
    own, tile = stored_density_blocks.shape[:2]
    capacity = device_request.shape[2]
    slots = devs * own
    atoms = atom_xyz.shape[1]
    half, quarter = own // 2, own // 4
    request = device_request
    dma = pltpu.SemaphoreType.DMA

    density, own_rows, table = pl.pallas_call(
        functools.partial(density_kernel, groups, devs, capacity),
        out_shape=(
            jax.ShapeDtypeStruct((batches, points), F32),
            jax.ShapeDtypeStruct((batches, LANES), F32),
            jax.ShapeDtypeStruct((devs * groups, batches, LANES), F32),
        ),
        in_specs=[VMEM, SMEM, SMEM, SMEM, VMEM, VMEM, VMEM, ANY],
        out_specs=(VMEM, VMEM, VMEM),
        scratch_shapes=[
            pltpu.VMEM((batches, points, width), BF16),
            pltpu.VMEM((slots, tile, tile), BF16),
            pltpu.VMEM((devs, groups, batches, LANES), F32),
            dma((2,)),
            dma((devs,)),
            dma((devs,)),
            dma((devs,)),
            dma((devs,)),
            dma((devs,)),
            dma((devs,)),
            dma((groups,)),
            dma((groups,)),
            dma((devs,)),
            dma((devs,)),
        ],
        compiler_params=pltpu.CompilerParams(collective_id=0, has_side_effects=True),
    )(
        stored_density_blocks,
        request,
        batch_blocks,
        batch_atom,
        point_offset,
        point_weight,
        atom_xyz,
        basis_values,
    )

    part, multipoles, density = pl.pallas_call(
        functools.partial(term_kernel, capacity, own),
        out_shape=(
            jax.ShapeDtypeStruct((slots, tile, tile), BF16),
            jax.ShapeDtypeStruct((4, atoms), F32),
            jax.ShapeDtypeStruct((batches, points), F32),
        ),
        in_specs=[SMEM, SMEM, VMEM, VMEM, VMEM, VMEM, VMEM, VMEM, VMEM],
        out_specs=(VMEM, VMEM, VMEM),
        scratch_shapes=[pltpu.VMEM((slots, tile, tile), F32)],
    )(
        request,
        batch_blocks,
        basis_values,
        table,
        own_rows,
        density,
        point_weight,
        exchange_kernel,
        point_offset,
    )

    hamiltonian = pl.pallas_call(
        functools.partial(reduce_kernel, groups, devs),
        out_shape=jax.ShapeDtypeStruct((own, tile, tile), BF16),
        in_specs=[VMEM],
        out_specs=VMEM,
        scratch_shapes=[
            pltpu.VMEM((devs, half, tile, tile), BF16),
            pltpu.VMEM((devs, quarter, tile, tile), BF16),
            pltpu.VMEM((devs, quarter, tile, tile), BF16),
            pltpu.VMEM((devs, quarter, tile, tile), BF16),
            pltpu.VMEM((devs, quarter, tile, tile), BF16),
            pltpu.VMEM((groups // 4, quarter, tile, tile), BF16),
            pltpu.VMEM((own, tile, tile), BF16),
            dma((devs,)),
            dma((devs,)),
            dma((devs,)),
            dma((devs,)),
            dma((devs,)),
            dma((devs,)),
            dma((groups // 4,)),
            dma((groups // 4,)),
            dma((2,)),
            dma((2,)),
        ],
        compiler_params=pltpu.CompilerParams(collective_id=1, has_side_effects=True),
    )(part)
    return (hamiltonian, density, multipoles)


def solution(mesh):
    return jax.shard_map(
        functools.partial(on_device, mesh.shape["grp"], mesh.shape["dev"]),
        mesh=mesh,
        in_specs=(
            P(("grp", "dev"), None, None),
            P("dev", None, None),
            P(("grp", "dev"), None, None),
            P(("grp", "dev"), None),
            P(("grp", "dev")),
            P(None, ("grp", "dev"), None),
            P(("grp", "dev"), None),
            P(("grp", "dev"), None),
            P(),
        ),
        out_specs=(P("dev", None, None), P(("grp", "dev"), None), P()),
        check_vma=False,
    )
```

```python
import functools

import jax
import jax.numpy as jnp
from jax import lax
from jax.experimental import pallas as pl
from jax.experimental.pallas import tpu as pltpu
from jax.sharding import PartitionSpec as P

MESH = pl.DeviceIdType.MESH
LANES = 128
VMEM = pl.BlockSpec(memory_space=pltpu.VMEM)
SMEM = pl.BlockSpec(memory_space=pltpu.SMEM)
ANY = pl.BlockSpec(memory_space=pl.ANY)
F32 = jnp.float32
BF16 = jnp.bfloat16


def remote(src, dst, send, recv, grp, dev):
    return pltpu.make_async_remote_copy(
        src_ref=src,
        dst_ref=dst,
        send_sem=send,
        recv_sem=recv,
        device_id=(grp, dev),
        device_id_type=MESH,
    )


def meet(peers):
    barrier = pltpu.get_barrier_semaphore()
    for grp, dev in peers:
        pl.semaphore_signal(barrier, inc=1, device_id=(grp, dev), device_id_type=MESH)
    pl.semaphore_wait(barrier, len(peers))


def slot_of(request, blocks, b, p, capacity, own):
    position = blocks[b, p]
    owner = position // capacity
    return owner * own + request[0, owner, position - owner * capacity]


def flip(index, mask):
    out = index
    bit = 1
    while bit <= mask:
        if mask & bit:
            out = out + bit - 2 * bit * lax.rem(index // bit, 2)
        bit *= 2
    return out


def density_kernel(
    groups,
    devs,
    capacity,
    stored,
    request,
    blocks,
    batch_atom,
    offset,
    weight,
    xyz,
    values_any,
    density,
    own_rows,
    table_out,
    values,
    gathered,
    table,
    local_sem,
    send_a,
    recv_a,
    send_y,
    recv_y,
    send_b,
    recv_b,
    send_c,
    recv_c,
    send_d,
    recv_d,
):
    g, me = lax.axis_index("grp"), lax.axis_index("dev")
    own, tile = stored.shape[0], stored.shape[1]
    batches, points, width = values.shape
    rel = width // tile
    atoms = xyz.shape[1]
    half, quarter = own // 2, own // 4
    first_row = lax.rem(g, 2) * half
    lane_row = first_row + lax.rem(g // 2, 2) * quarter

    load = pltpu.make_async_copy(values_any, values, local_sem.at[0])
    load.start()
    mine = pltpu.make_async_copy(
        stored, gathered.at[pl.ds(me * own, own)], local_sem.at[1]
    )
    mine.start()
    peers = [(g, lax.rem(me + k, devs)) for k in range(1, devs)]
    peers += [(lax.rem(g + j, groups), me) for j in range(1, groups)]
    meet(peers)

    def piece(k):
        return pl.ds(flip(me, k) * own + lane_row, quarter)

    def source(k):
        return stored.at[pl.ds(lane_row, quarter)] if k == 0 else gathered.at[piece(k)]

    came = {}

    def onward(k):
        came[k + 1] = remote(
            source(k),
            gathered.at[piece(k)],
            send_a.at[k + 1],
            recv_a.at[k + 1],
            g,
            flip(me, 1),
        )
        came[k + 1].start()

    onward(0)
    for k in range(2, devs, 2):
        came[k] = remote(
            source(0), gathered.at[piece(0)], send_a.at[k], recv_a.at[k], g, flip(me, k)
        )
        came[k].start()

    centres = []
    spot = lax.broadcasted_iota(jnp.int32, (3, atoms), 1)
    for b in range(batches):
        centres.append(
            jnp.sum(jnp.where(spot == batch_atom[b], xyz[...], 0.0), axis=1, keepdims=True)
        )

    order = []
    for k in range(2, devs, 2):
        order += [k, k - 1]
    order.append(devs - 1)
    sideways, passed = {}, []

    def hand_over(k):
        sideways[k].wait_recv()
        rows = pl.ds(flip(me, k) * own + first_row, half)
        copy = remote(
            gathered.at[rows], gathered.at[rows], send_b.at[k], recv_b.at[k], flip(g, 1), me
        )
        copy.start()
        passed.append(copy)

    for step, k in enumerate(order):
        came[k].wait_recv()
        sideways[k] = remote(
            gathered.at[piece(k)],
            gathered.at[piece(k)],
            send_y.at[k],
            recv_y.at[k],
            flip(g, 2),
            me,
        )
        sideways[k].start()
        if k % 2 == 0:
            onward(k)
        if step >= 2:
            hand_over(order[step - 2])
    for k in order[-2:]:
        hand_over(k)
    out = list(came.values()) + list(sideways.values())
    load.wait()
    mine.wait()
    for copy in passed:
        copy.wait_recv()

    lane = lax.broadcasted_iota(jnp.int32, (1, LANES), 1)
    for b in range(batches):
        matrix = jnp.concatenate(
            [
                jnp.concatenate(
                    [
                        gathered[slot_of(request, blocks, b, i * rel + j, capacity, own)]
                        for j in range(rel)
                    ],
                    axis=1,
                )
                for i in range(rel)
            ],
            axis=0,
        )
        left = jnp.dot(values[b], matrix, preferred_element_type=F32)
        product = left * values[b].astype(F32)
        folded = product[:, :tile]
        for i in range(1, rel):
            folded = folded + product[:, i * tile : (i + 1) * tile]
        row = jnp.sum(folded.T, axis=0, keepdims=True)
        density[pl.ds(b, 1), :] = row
        weighted = row * weight[pl.ds(b, 1), :]
        parts = [jnp.sum(weighted, axis=1, keepdims=True)]
        for k in range(3):
            parts.append(
                jnp.sum(weighted * offset[k, pl.ds(b, 1), :], axis=1, keepdims=True)
            )
        parts += [centres[b][k : k + 1] for k in range(3)]
        entry = jnp.zeros((1, LANES), F32) + batch_atom[b].astype(F32)
        for k, part in enumerate(parts):
            entry = jnp.where(lane == k, part, entry)
        own_rows[pl.ds(b, 1), :] = entry
        table[me, g, pl.ds(b, 1), :] = entry

    first = []
    for j in range(1, groups):
        copy = remote(
            table.at[me, g],
            table.at[me, g],
            send_c.at[j],
            recv_c.at[j],
            lax.rem(g + j, groups),
            me,
        )
        copy.start()
        first.append(copy)
    for copy in first:
        copy.wait_recv()
    second = []
    for k in range(1, devs):
        copy = remote(
            table.at[me], table.at[me], send_d.at[k], recv_d.at[k], g, lax.rem(me + k, devs)
        )
        copy.start()
        second.append(copy)
    for copy in out + passed + first:
        copy.wait_send()
    for copy in second:
        copy.wait_recv()
    for copy in second:
        copy.wait_send()
    for d in range(devs):
        table_out[d * groups : (d + 1) * groups] = table[d]


def term_kernel(
    capacity,
    own,
    request,
    blocks,
    values,
    table,
    own_rows,
    density,
    weight,
    exchange,
    offset,
    part,
    multipoles,
    density_out,
    total,
):
    batches, points, width = values.shape
    tile = part.shape[1]
    rel = width // tile
    devices = table.shape[0]
    atoms = multipoles.shape[1]
    chunk = min(devices, 32)
    total[...] = jnp.zeros_like(total)
    density_out[...] = density[...]

    places = [
        [own_rows[pl.ds(b, 1), 4 + k : 5 + k] + offset[k, pl.ds(b, 1), :] for k in range(3)]
        for b in range(batches)
    ]
    spot = lax.broadcasted_iota(jnp.int32, (1, atoms), 1).astype(F32)

    def gather(step, carry):
        fields, moments = carry
        fields, moments = list(fields), list(moments)
        for source in range(batches):
            rows = table[pl.ds(step * chunk, chunk), source, :]
            column = [rows[:, k : k + 1] for k in range(8)]
            hit = column[7] == spot
            for k in range(4):
                moments[k] = moments[k] + jnp.sum(
                    jnp.where(hit, column[k], 0.0), axis=0, keepdims=True
                )
            for b in range(batches):
                gap = [places[b][k] - column[4 + k] for k in range(3)]
                inverse = lax.rsqrt(
                    gap[0] * gap[0] + gap[1] * gap[1] + gap[2] * gap[2] + 1.0
                )
                cube = inverse * inverse * inverse
                dipole = column[1] * gap[0] + column[2] * gap[1] + column[3] * gap[2]
                fields[b] = fields[b] + jnp.sum(
                    column[0] * inverse + dipole * cube, axis=0, keepdims=True
                )
        return tuple(fields), tuple(moments)

    carry = (
        tuple(jnp.zeros((1, points), F32) for _ in range(batches)),
        tuple(jnp.zeros((1, atoms), F32) for _ in range(4)),
    )
    if devices == chunk:
        fields, moments = gather(0, carry)
    else:
        fields, moments = lax.fori_loop(0, devices // chunk, gather, carry)
    for k in range(4):
        multipoles[pl.ds(k, 1), :] = moments[k]

    for b in range(batches):
        pick = pl.ds(b, 1)
        factors = (
            weight[pick, :] * exchange[pick, :] * density[pick, :],
            weight[pick, :] * fields[b],
        )
        wide = values[b].astype(F32)
        scaled = []
        for factor in factors:
            column = jnp.broadcast_to(factor, (tile, points)).T
            scaled.append(
                jnp.concatenate(
                    [
                        (wide[:, i * tile : (i + 1) * tile] * column).astype(BF16)
                        for i in range(rel)
                    ],
                    axis=1,
                )
            )
        stacked = jnp.concatenate(scaled, axis=0)
        doubled = jnp.concatenate([values[b], values[b]], axis=0)
        term = lax.dot_general(
            stacked, doubled, (((0,), (0,)), ((), ())), preferred_element_type=F32
        )
        for i in range(rel):
            for j in range(rel):
                slot = slot_of(request, blocks, b, i * rel + j, capacity, own)
                total[slot] += term[i * tile : (i + 1) * tile, j * tile : (j + 1) * tile]
    part[...] = total[...].astype(BF16)


def reduce_kernel(
    groups,
    devs,
    part,
    result,
    paired,
    sent_1,
    came_1,
    sent_2,
    came_2,
    outgoing,
    arrived,
    across,
    final,
    send_a,
    recv_a,
    send_1,
    recv_1,
    send_2,
    recv_2,
    send_b,
    recv_b,
    send_c,
    recv_c,
    send_d,
    recv_d,
):
    g, me = lax.axis_index("grp"), lax.axis_index("dev")
    own = result.shape[0]
    half, quarter = own // 2, own // 4
    quads = groups // 4
    quad, lane = g // 4, lax.rem(g, 4)
    core, side = lax.rem(g, 2), lax.rem(g // 2, 2)
    pair, beside = flip(g, 1), flip(g, 2)
    turn_y, turn_x = 1 - 2 * side, 1 - 2 * lax.rem(me, 2)
    one = (g + (1 - core) * 2 * turn_y, me + core * turn_x)
    two = (g + core * 2 * turn_y, me + (1 - core) * turn_x)

    peers = [(pair, me), (beside, me)]
    peers += [(g, flip(me, k)) for k in [1, *range(2, devs, 2)]]
    peers += [(lax.rem(quad + j, quads) * 4 + lane, me) for j in range(1, quads)]
    meet(peers)

    order = list(range(devs - 1, -1, -1))
    halves, first, second, out = {}, {}, {}, {}
    for k in order:
        halves[k] = remote(
            part.at[pl.ds(flip(me, k) * own + (1 - core) * half, half)],
            paired.at[k],
            send_a.at[k],
            recv_a.at[k],
            pair,
            me,
        )
        halves[k].start()

    def of_pair(a, b, k):
        over_x = core * a + (1 - core) * b
        which = side + ((1 - core) * a + core * b) * turn_y
        row = (flip(me, k) + over_x * turn_x) * own + core * half + which * quarter
        here = part[pl.ds(row, quarter)]
        there = paired[k + over_x, pl.ds(which * quarter, quarter)]
        return here.astype(F32) + there.astype(F32)

    def of_four(b, k):
        first[k + b].wait_recv()
        return of_pair(0, b, k) + came_1[k + b].astype(F32)

    def of_eight(k):
        second[k].wait_recv()
        return of_four(0, k) + came_2[k // 2].astype(F32)

    def step_1(k):
        halves[k + 1].wait_recv()
        halves[k].wait_recv()
        for b in (1, 0):
            slot = k + b
            sent_1[slot] = of_pair(1, b, k).astype(BF16)
            first[slot] = remote(
                sent_1.at[slot], came_1.at[slot], send_1.at[slot], recv_1.at[slot], *one
            )
            first[slot].start()

    def step_2(k):
        slot = k // 2
        sent_2[slot] = of_four(1, k).astype(BF16)
        second[k] = remote(
            sent_2.at[slot], came_2.at[slot], send_2.at[slot], recv_2.at[slot], *two
        )
        second[k].start()

    def step_3(k):
        slot = k // 2
        outgoing[slot] = of_eight(k).astype(BF16)
        out[k] = remote(
            outgoing.at[slot],
            arrived.at[slot],
            send_b.at[slot],
            recv_b.at[slot],
            g,
            flip(me, k),
        )
        out[k].start()

    planes = list(range(devs - 2, -1, -2))
    for step, k in enumerate(planes):
        step_1(k)
        if step >= 1:
            step_2(planes[step - 1])
        if step >= 2:
            step_3(planes[step - 2])
    step_2(0)
    for k in planes[-2:-1]:
        step_3(k)
    whole = of_eight(0)
    for k in planes[:-1]:
        out[k].wait_recv()
        whole = whole + arrived[k // 2].astype(F32)
    others = []
    if quads > 1:
        across[quad] = whole.astype(BF16)
        for j in range(1, quads):
            copy = remote(
                across.at[quad],
                across.at[quad],
                send_c.at[j],
                recv_c.at[j],
                lax.rem(quad + j, quads) * 4 + lane,
                me,
            )
            copy.start()
            others.append(copy)
        for copy in others:
            copy.wait_recv()
        whole = across[0].astype(F32)
        for j in range(1, quads):
            whole = whole + across[j].astype(F32)
    part_rows = pl.ds(core * half + side * quarter, quarter)
    half_rows = pl.ds(core * half, half)
    final[part_rows] = whole.astype(BF16)
    for step, (where, to) in enumerate(((part_rows, beside), (half_rows, pair))):
        copy = remote(
            final.at[where], final.at[where], send_d.at[step], recv_d.at[step], to, me
        )
        copy.start()
        copy.wait_recv()
        others.append(copy)
    for copy in [*halves.values(), *first.values(), *second.values(), *out.values(), *others]:
        copy.wait_send()
    result[...] = final[...]


def on_device(
    groups,
    devs,
    basis_values,
    stored_density_blocks,
    device_request,
    batch_blocks,
    batch_atom,
    point_offset,
    point_weight,
    exchange_kernel,
    atom_xyz,
):
    batches, points, width = basis_values.shape
    own, tile = stored_density_blocks.shape[:2]
    capacity = device_request.shape[2]
    slots = devs * own
    atoms = atom_xyz.shape[1]
    half, quarter = own // 2, own // 4
    request = device_request
    dma = pltpu.SemaphoreType.DMA

    density, own_rows, table = pl.pallas_call(
        functools.partial(density_kernel, groups, devs, capacity),
        out_shape=(
            jax.ShapeDtypeStruct((batches, points), F32),
            jax.ShapeDtypeStruct((batches, LANES), F32),
            jax.ShapeDtypeStruct((devs * groups, batches, LANES), F32),
        ),
        in_specs=[VMEM, SMEM, SMEM, SMEM, VMEM, VMEM, VMEM, ANY],
        out_specs=(VMEM, VMEM, VMEM),
        scratch_shapes=[
            pltpu.VMEM((batches, points, width), BF16),
            pltpu.VMEM((slots, tile, tile), BF16),
            pltpu.VMEM((devs, groups, batches, LANES), F32),
            dma((2,)),
            dma((devs,)),
            dma((devs,)),
            dma((devs,)),
            dma((devs,)),
            dma((devs,)),
            dma((devs,)),
            dma((groups,)),
            dma((groups,)),
            dma((devs,)),
            dma((devs,)),
        ],
        compiler_params=pltpu.CompilerParams(collective_id=0, has_side_effects=True),
    )(
        stored_density_blocks,
        request,
        batch_blocks,
        batch_atom,
        point_offset,
        point_weight,
        atom_xyz,
        basis_values,
    )

    part, multipoles, density = pl.pallas_call(
        functools.partial(term_kernel, capacity, own),
        out_shape=(
            jax.ShapeDtypeStruct((slots, tile, tile), BF16),
            jax.ShapeDtypeStruct((4, atoms), F32),
            jax.ShapeDtypeStruct((batches, points), F32),
        ),
        in_specs=[SMEM, SMEM, VMEM, VMEM, VMEM, VMEM, VMEM, VMEM, VMEM],
        out_specs=(VMEM, VMEM, VMEM),
        scratch_shapes=[pltpu.VMEM((slots, tile, tile), F32)],
    )(
        request,
        batch_blocks,
        basis_values,
        table,
        own_rows,
        density,
        point_weight,
        exchange_kernel,
        point_offset,
    )

    hamiltonian = pl.pallas_call(
        functools.partial(reduce_kernel, groups, devs),
        out_shape=jax.ShapeDtypeStruct((own, tile, tile), BF16),
        in_specs=[VMEM],
        out_specs=VMEM,
        scratch_shapes=[
            pltpu.VMEM((devs, half, tile, tile), BF16),
            pltpu.VMEM((devs, quarter, tile, tile), BF16),
            pltpu.VMEM((devs, quarter, tile, tile), BF16),
            pltpu.VMEM((devs // 2, quarter, tile, tile), BF16),
            pltpu.VMEM((devs // 2, quarter, tile, tile), BF16),
            pltpu.VMEM((devs // 2, quarter, tile, tile), BF16),
            pltpu.VMEM((devs // 2, quarter, tile, tile), BF16),
            pltpu.VMEM((groups // 4, quarter, tile, tile), BF16),
            pltpu.VMEM((own, tile, tile), BF16),
            dma((devs,)),
            dma((devs,)),
            dma((devs,)),
            dma((devs,)),
            dma((devs,)),
            dma((devs,)),
            dma((devs,)),
            dma((devs,)),
            dma((groups // 4,)),
            dma((groups // 4,)),
            dma((2,)),
            dma((2,)),
        ],
        compiler_params=pltpu.CompilerParams(collective_id=1, has_side_effects=True),
    )(part)
    return (hamiltonian, density, multipoles)


def solution(mesh):
    return jax.shard_map(
        functools.partial(on_device, mesh.shape["grp"], mesh.shape["dev"]),
        mesh=mesh,
        in_specs=(
            P(("grp", "dev"), None, None),
            P("dev", None, None),
            P(("grp", "dev"), None, None),
            P(("grp", "dev"), None),
            P(("grp", "dev")),
            P(None, ("grp", "dev"), None),
            P(("grp", "dev"), None),
            P(("grp", "dev"), None),
            P(),
        ),
        out_specs=(P("dev", None, None), P(("grp", "dev"), None), P()),
        check_vma=False,
    )
```
